32 devices in a mesh: row: 4 (over y, x), col: 8 (over z, core).
Axes of the slice: x: 2, y: 2, z: 4, core: 2. Of those that a mesh axis runs over, the one named last changes fastest.
Arguments:
- fire_state: float32 [64, 192, 1024], P(None, 'row', 'col'), may hold values from -6 to 6
- fuel_class: int32 [192, 1024], P('row', 'col'), may hold values from 0 to 12
- firebreak: int32 [192, 1024], P('row', 'col'), may hold values 0 or 1
- ignition: int32 [192, 1024], P('row', 'col'), may hold values 0 or 1
- spread_rate: float32 [13, 64], replicated, may hold values from 0.03 to 0.12
- spread_rows: float32 [64, 64], replicated, may hold values from -0.375 to 0.375
- spread_cols: float32 [64, 64], replicated, may hold values from -0.375 to 0.375
- reaction: float32 [64, 64], replicated, may hold values from -0.75 to 0.75
- ignition_heat: float32 [64], replicated, may hold values from -4 to 4
Outputs:
- final_state: float32 [64, 192, 1024], P(None, 'row', 'col')
The draws below stay inside these ranges and needn't reach their ends.
All inputs are finite; a program needn't handle non-finite values. No bound on the sum of `firebreak` or of `ignition` on one device may be relied on, other than what follows from the above.
Results may differ from the reference program's by a relative error of at most 0.0003.
Values sent between devices are 32-bit elements; how exact they have to be, the bound alone decides.
A program may use at most 64 MiB of HBM per device.

```python
import math
import jax
import jax.numpy as jnp
from jax import lax

C = 64
K = 13
W_DEV = 128
ITERS = 4
NX = 192
NY = 1024


def touch_ends(drawn, stream_key, low, largest):
    index_at = [jax.random.randint(jax.random.fold_in(stream_key, axis), (), 0, length) for axis, length in enumerate(drawn.shape)]
    main_axis = drawn.shape.index(max(drawn.shape))
    beside = index_at[:main_axis] + [(index_at[main_axis] + 1) % drawn.shape[main_axis]] + index_at[main_axis + 1:]
    return drawn.at[tuple(index_at)].set(low).at[tuple(beside)].set(largest)


def shard_levels(stream_key, dims, shards, smallest, high):
    gain = 1.0
    for axis_at, blocks in shards:
        heights = jax.random.uniform(jax.random.fold_in(jax.random.fold_in(stream_key, 6), axis_at), (blocks,), jnp.float32, smallest / len(shards), high / len(shards))
        gain = gain * jnp.repeat(jnp.exp(heights), dims[axis_at] // blocks).reshape((-1,) + (1,) * (len(dims) - 1 - axis_at))
    return gain


def centred(rng, dims, scale, reach, cuts=(), kind=jnp.bfloat16):
    array = jax.random.normal(rng, dims, jnp.float32) * scale
    if len(cuts) > 0:
        array = shard_levels(rng, dims, cuts, -0.22, 0.18) * array
    return jnp.clip(array, min=-reach, max=reach).astype(kind)


def setup_inputs(seed: int = 0) -> dict:
    key_list = jax.random.split(jax.random.key(seed), 10)
    fire_state = centred(key_list[0], (C, NX, NY), 1.0, 6.0, ((1, 4), (2, 8)), jnp.float32)
    fuel_class = touch_ends(jax.random.randint(key_list[1], (NX, NY), 0, K), jax.random.fold_in(key_list[1], 1), 0, K - 1).astype(jnp.int32)
    firebreak = touch_ends((jax.random.randint(key_list[2], (NX, NY), 0, 8) < 1).astype(jnp.int32), jax.random.fold_in(key_list[2], 1), 0, 1)
    ignition = touch_ends((jax.random.randint(key_list[3], (NX, NY), 0, 16) < 1).astype(jnp.int32), jax.random.fold_in(key_list[3], 1), 0, 1)
    spread_rate = jnp.clip(jnp.exp(jax.random.uniform(key_list[4], (K, C), jnp.float32, math.log(0.03), math.log(0.12))), 0.03, 0.12)
    spread_rows = centred(key_list[5], (C, C), (4 * C) ** -0.5, 0.375, (), jnp.float32)
    spread_cols = centred(key_list[6], (C, C), (4 * C) ** -0.5, 0.375, (), jnp.float32)
    reaction = centred(key_list[7], (C, C), C ** -0.5, 0.75, (), jnp.float32)
    ignition_heat = centred(key_list[8], (C,), 1.0, 4.0, (), jnp.float32)
    return dict(fire_state=fire_state, fuel_class=fuel_class, firebreak=firebreak, ignition=ignition, spread_rate=spread_rate, spread_rows=spread_rows, spread_cols=spread_cols, reaction=reaction, ignition_heat=ignition_heat)


def mixing(matrix, values):
    return jnp.einsum('dc,chw->dhw', matrix, values, precision=lax.Precision.HIGHEST)


def tendency(padded, burnable, spread, heating, spread_rows, spread_cols, reaction):
    center = padded[:, 1:-1, 1:-1]
    vertical = padded[:, :-2, 1:-1] + padded[:, 2:, 1:-1] - 2.0 * center
    horizontal = padded[:, 1:-1, :-2] + padded[:, 1:-1, 2:] - 2.0 * center
    mixed = vertical + mixing(spread_rows, vertical) + horizontal + mixing(spread_cols, horizontal)
    drive = spread * mixed + mixing(reaction, jnp.tanh(center)) + heating
    return burnable[None] * drive - 0.5 * center


def full_tendency(field, burnable_int, fuel_class, ignition, spread_rate, spread_rows, spread_cols, reaction, ignition_heat):
    padded = jnp.pad(field, ((0, 0), (1, 1), (1, 1)))
    blocks = NY // W_DEV

    def one_block(column_block):
        begin = column_block * W_DEV
        piece = lax.dynamic_slice_in_dim(padded, begin, W_DEV + 2, 2)
        burnable = lax.dynamic_slice_in_dim(burnable_int, begin, W_DEV, 1).astype(jnp.float32)
        fuel = lax.dynamic_slice_in_dim(fuel_class, begin, W_DEV, 1)
        lit = lax.dynamic_slice_in_dim(ignition, begin, W_DEV, 1).astype(jnp.float32)
        onehot = (fuel[None] == jnp.arange(K, dtype=jnp.int32)[:, None, None]).astype(jnp.float32)
        spread = jnp.einsum('kc,khw->chw', spread_rate, onehot, precision=lax.Precision.HIGHEST)
        heating = lit[None] * ignition_heat[:, None, None]
        return tendency(piece, burnable, spread, heating, spread_rows, spread_cols, reaction)

    result = lax.map(one_block, jnp.arange(blocks, dtype=jnp.int32))
    result = jnp.moveaxis(result, 0, 2)
    return result.reshape(C, NX, NY)


def reference(fire_state, fuel_class, firebreak, ignition, spread_rate, spread_rows, spread_cols, reaction, ignition_heat):
    burnable_int = 1 - firebreak
    field = fire_state
    for iteration in range(ITERS):
        first = full_tendency(field, burnable_int, fuel_class, ignition, spread_rate, spread_rows, spread_cols, reaction, ignition_heat)
        middle = field + first
        second = full_tendency(middle, burnable_int, fuel_class, ignition, spread_rate, spread_rows, spread_cols, reaction, ignition_heat)
        field = field + 0.5 * (first + second)
    return field
```

```python
import functools

import jax
import jax.numpy as jnp
from jax import lax
from jax.experimental import pallas as pl
from jax.experimental.pallas import tpu as pltpu
from jax.sharding import PartitionSpec as P

ITERS = 4
DEPTH = 2 * ITERS
PAD = 8
BLOCK = 4
CHUNK = 4
BF16, F32 = jnp.bfloat16, jnp.float32
MESH = pl.DeviceIdType.MESH


def split(x):
    high = x.astype(BF16)
    return high, (x - high.astype(F32)).astype(BF16)


def dot(a, b):
    return jnp.dot(a, b, preferred_element_type=F32)


def lanes(shape):
    return lax.broadcasted_iota(jnp.int32, shape, 1)


def rows_of(shape):
    return lax.broadcasted_iota(jnp.int32, shape, 0)


def on_diagonal(matrix):
    c = matrix.shape[0]
    turned = matrix.T
    wide = jnp.concatenate([turned, turned], axis=1)
    first = lanes(wide.shape) < c
    return jnp.concatenate([jnp.where(first, wide, 0.0), jnp.where(first, 0.0, wide)], axis=0)


def kernel(
    dims,
    x_hbm, fuel_hbm, break_hbm, lit_hbm, rate_hbm, srow_hbm, scol_hbm, react_hbm, heat_hbm,
    out_ref,
    x_ref, fuel_ref, break_ref, lit_ref, rate_ref, srow_ref, scol_ref, react_ref, heat_ref, load_sem,
    v, mid, coef, burn, heat, ws, wa, wc, halo_x, flat_send, flat_recv,
    row_send, row_recv, int_send, int_recv, col_send, col_recv, flat_ssem, flat_rsem, corner_send, corner_recv,
):
    n_row, n_col, c, h, w, k8 = dims
    d = DEPTH
    own = h // 2
    total = own + d
    wide = w + 2 * d
    two = 2 * c
    r, q = lax.axis_index("row"), lax.axis_index("col")
    partner = ({"row": r - 1}, {"row": r + 1}, {"col": q - 1}, {"col": q + 1})
    has = (r > 0, r < n_row - 1, q > 0, q < n_col - 1)

    def load(n, src, dst):
        return pltpu.make_async_copy(src, dst, load_sem.at[n])

    body = pl.ds(d, h)
    cell_loads = [
        load(0, fuel_hbm, fuel_ref.at[body]), load(1, break_hbm, break_ref.at[body]), load(2, lit_hbm, lit_ref.at[body]),
        load(3, rate_hbm, rate_ref), load(4, heat_hbm, heat_ref),
    ]
    weight_loads = [load(5, srow_hbm, srow_ref), load(6, scol_hbm, scol_ref), load(7, react_hbm, react_ref)]
    field_load = load(8, x_hbm, x_ref.reshape(c, h, w))
    for one in [field_load] + cell_loads + weight_loads:
        one.start()

    for at in (pl.ds(0, d), pl.ds(h + d, d)):
        fuel_ref[at] = jnp.zeros((d, w), jnp.int32)
        lit_ref[at] = jnp.zeros((d, w), jnp.int32)
        break_ref[at] = jnp.ones((d, w), jnp.int32)
    flat_recv[...] = jnp.ones_like(flat_recv)
    halo_x[...] = jnp.zeros_like(halo_x)
    v[:, PAD:PAD + d] = jnp.zeros((total + 1, d, two), F32)
    v[:, PAD + d + w:PAD + wide] = jnp.zeros((total + 1, d, two), F32)

    barrier = pltpu.get_barrier_semaphore()
    for s in range(4):
        @pl.when(has[s])
        def _(s=s):
            pl.semaphore_signal(barrier, inc=1, device_id=partner[s], device_id_type=MESH)

    def remote(src, dst, send_sem, recv_sem, s):
        return pltpu.make_async_remote_copy(
            src_ref=src, dst_ref=dst, send_sem=send_sem, recv_sem=recv_sem, device_id=partner[s], device_id_type=MESH
        )

    def int_copy(n, s):
        src = (fuel_hbm, break_hbm, lit_hbm)[n]
        dst = (fuel_ref, break_ref, lit_ref)[n]
        from_row, to_row = (0, h + d) if s == 0 else (h - d, 0)
        return remote(src.at[pl.ds(from_row, d)], dst.at[pl.ds(to_row, d)], int_send.at[n, s], int_recv.at[n, s], s)

    def row_copy(j, s):
        src, at = (j, d - 1 - j) if s == 0 else (h - 1 - j, d - 1 - j)
        return remote(x_hbm.at[:, src, :], halo_x.at[s, at], row_send.at[j, s], row_recv.at[j, s], s)

    def edge(s, at):
        if s == 2:
            return v.at[at, PAD + d:PAD + 2 * d], v.at[at, PAD + d + w:PAD + wide]
        return v.at[at, PAD + w:PAD + w + d], v.at[at, PAD:PAD + d]

    def col_copy(s):
        src, dst = edge(s, pl.ds(d, own))
        return remote(src, dst, col_send.at[s - 2], col_recv.at[s - 2], s)

    def corner_copy(j, s):
        src, dst = edge(s, pl.ds(d - CHUNK * (j + 1), CHUNK))
        return remote(src, dst, corner_send.at[j, s - 2], corner_recv.at[j, s - 2], s)

    def flat_copy(s):
        return remote(flat_send.at[s - 2], flat_recv.at[s - 2], flat_ssem.at[s - 2], flat_rsem.at[s - 2], s)

    def start(make, s):
        @pl.when(has[s])
        def _():
            make(s).start()

    def sent(make, s):
        @pl.when(has[s])
        def _():
            make(s).wait_send()

    def arrived(make, s):
        @pl.when(has[s ^ 1])
        def _():
            make(s).wait_recv()

    n_near = sum(s.astype(jnp.int32) for s in has)
    pl.semaphore_wait(barrier, n_near)
    for s in range(2):
        for n in range(3):
            start(functools.partial(int_copy, n), s)
    for j in range(d):
        for s in range(2):
            start(functools.partial(row_copy, j), s)

    for one in weight_loads:
        one.wait()
    row_hi, row_lo = split(on_diagonal(srow_ref[...]))
    col_hi, col_lo = split(on_diagonal(scol_ref[...]))
    rea_hi, rea_lo = split(on_diagonal(react_ref[...]))
    ws[0:two] = jnp.concatenate([row_hi, row_lo], axis=1)
    ws[two:2 * two] = jnp.concatenate([col_hi, col_lo], axis=1)
    wa[0:two] = jnp.concatenate([rea_hi, rea_lo], axis=1)
    wa[two:2 * two] = jnp.concatenate([rea_hi, jnp.zeros_like(rea_lo)], axis=1)

    field_load.wait()

    def turn_in(i, carry):
        tall = jnp.concatenate([x_ref[pl.ds(i, c, stride=h), :], x_ref[pl.ds(h - 1 - i, c, stride=h), :]], axis=0)
        v[d + i, PAD + d:PAD + d + w] = tall.T
        return carry

    lax.fori_loop(0, own, turn_in, 0, unroll=4)
    for s in (2, 3):
        start(col_copy, s)

    for one in cell_loads:
        one.wait()
    for s in range(2):
        for n in range(3):
            arrived(functools.partial(int_copy, n), s)

    group = w // d
    lane = lanes((w, 2 * w))
    from_col = lax.rem(lane, d) + jnp.where(lane < w, 0, w - d)
    pick = jnp.where(rows_of((w, 2 * w)) == from_col, 1.0, 0.0).astype(BF16)
    ints = [ref[...].astype(F32) for ref in (fuel_ref, break_ref, lit_ref)]
    spread_out = dot(jnp.concatenate(ints, axis=0).astype(BF16), pick)
    slot = lax.rem(lanes((group, 2 * w)), w) // d
    ups = rows_of((group, 2 * w)) == slot
    downs = (group - 1) - rows_of((group, 2 * w)) == slot
    full = h + 2 * d
    for g in range(total // group):
        lines = []
        for half in range(2):
            for n in range(3):
                first = n * full + (g * group if half == 0 else full - (g + 1) * group)
                piece = jnp.where(ups if half == 0 else downs, spread_out[first:first + group], 0.0)
                lines.append(jnp.sum(piece, axis=0, keepdims=True))
        lines.append(jnp.zeros((2, 2 * w), F32))
        packed = jnp.concatenate(lines, axis=0)
        flat_send[0, g] = packed[:, :w]
        flat_send[1, g] = packed[:, w:]
    for s in (2, 3):
        start(flat_copy, s)

    k = rate_ref.shape[0]
    part = k8 + 8
    rates = jnp.concatenate([rate_ref[...], rate_ref[...]], axis=1)
    heats = jnp.concatenate([heat_ref[...], heat_ref[...]], axis=1)
    wc[...] = jnp.zeros_like(wc)
    for s in range(2):
        mine = (lanes((1, two)) < c) if s == 0 else (lanes((1, two)) >= c)
        wc[s * part:s * part + k, 0:two] = jnp.where(mine, rates, 0.0)
        wc[s * part + k8:s * part + k8 + 1, two:2 * two] = jnp.where(mine, 1.0, 0.0)
        wc[s * part + k8 + 1:s * part + k8 + 2, 2 * two:3 * two] = jnp.where(mine, heats, 0.0)
    tables = jnp.concatenate(split(wc[...]), axis=0)
    classes, slots = rows_of((k8, w)).astype(F32), rows_of((8, w))

    def terms_of(pairs):
        parts = []
        for fuel, broken, lit in pairs:
            alive = 1.0 - broken
            parts.append(jnp.where(fuel == classes, alive, 0.0))
            parts.append(jnp.where(slots == 0, alive, jnp.where(slots == 1, alive * lit, 0.0)))
        tall = jnp.concatenate(parts + parts, axis=0)
        return dot(tall.T.astype(BF16), tables)

    def cells(p, carry):
        pairs = []
        for at in (pl.ds(p, 1), pl.ds(full - 1 - p, 1)):
            pairs.append([ref[at, :].astype(F32) for ref in (fuel_ref, break_ref, lit_ref)])
        terms = terms_of(pairs)
        for n, ref in enumerate((coef, burn, heat)):
            ref[p, d:d + w] = terms[:, n * two:(n + 1) * two]
        return carry

    lax.fori_loop(0, total, cells, 0, unroll=4)

    for s in (2, 3):
        arrived(flat_copy, s)
        arrived(col_copy, s)
    for s in (2, 3):
        to = d + w if s == 2 else 0
        for g in range(total // group):
            lines = flat_recv[s - 2, g]
            terms = terms_of([[lines[3 * half + n:3 * half + n + 1] for n in range(3)] for half in range(2)])
            for n, ref in enumerate((coef, burn, heat)):
                ref[g * group:(g + 1) * group, to:to + d] = terms[:, n * two:(n + 1) * two].reshape(group, d, two)
    for s in (2, 3):
        sent(col_copy, s)

    def evaluate(p, n, second, top=False):
        cur, target = (mid, v) if second else (v, mid)
        flat = lambda value: value.reshape(n * wide, two)
        inner = slice(PAD, PAD + wide)
        at = pl.ds(p, n)
        x = flat(cur[at, inner])
        above = flat(cur[pl.ds(p - 1, n), inner])
        if top:
            turned = pltpu.roll(cur[p + n - 1, inner], c, axis=1)
            below = jnp.concatenate([flat(cur[at, inner])[wide:], turned], axis=0)
        else:
            below = flat(cur[pl.ds(p + 1, n), inner])
        left = flat(cur[at, PAD - 1:PAD - 1 + wide])
        right = flat(cur[at, PAD + 1:PAD + 1 + wide])
        twice = x + x
        vertical = (above + below) - twice
        horizontal = (left + right) - twice
        coupled = dot(jnp.concatenate([vertical.astype(BF16), horizontal.astype(BF16)], axis=1), ws[...])
        hi, lo = split(jnp.tanh(x))
        burning = dot(jnp.concatenate([hi, lo], axis=1), wa[...])
        mixed = (vertical + horizontal) + (coupled[:, :two] + coupled[:, two:])
        fire = flat(coef[at]) * mixed + flat(burn[at]) * (burning[:, :two] + burning[:, two:])
        fire = (fire + flat(heat[at])) + 0.5 * x
        if second:
            fire = 0.5 * (fire + flat(v[at, inner]))
        target[at, inner] = fire.reshape(n, wide, two)

    def pyramid(i, carry):
        for s in range(4):
            second = s % 2 == 1
            low = d + 4 * i + s + 1
            top = 2 * BLOCK - 1 - s

            def block(b, carry):
                evaluate(low + b * BLOCK, BLOCK, second)
                return carry

            lax.fori_loop(0, own // BLOCK - 2 - i, block, 0)
            evaluate(total - top, top, second, top=True)
        return carry

    lax.fori_loop(0, ITERS // 2, pyramid, 0)

    for j in range(d // CHUNK):
        for m in range(j * CHUNK, (j + 1) * CHUNK):
            for s in range(2):
                arrived(functools.partial(row_copy, m), s)
        for m in range(CHUNK):
            p = d - CHUNK * (j + 1) + m
            v[p, PAD + d:PAD + d + w] = jnp.concatenate([halo_x[1, p], halo_x[0, p]], axis=0).T
        for s in (2, 3):
            start(functools.partial(corner_copy, j), s)
        for s in (2, 3):
            sent(functools.partial(corner_copy, j), s)
            arrived(functools.partial(corner_copy, j), s)

        def zone(t, carry):
            low = d - CHUNK * (j + 1) + 2 * t
            evaluate(low + 1, CHUNK, False)
            evaluate(low + 2, CHUNK, True)
            return carry

        lax.fori_loop(0, ITERS, zone, 0)

    def turn_out(i, carry):
        tall = v[d + i, PAD + d:PAD + d + w].T
        out_ref[pl.ds(i, c, stride=h), :] = tall[:c]
        out_ref[pl.ds(h - 1 - i, c, stride=h), :] = tall[c:]
        return carry

    lax.fori_loop(0, own, turn_out, 0, unroll=4)
    for s in range(2):
        for n in range(3):
            sent(functools.partial(int_copy, n), s)
        for j in range(d):
            sent(functools.partial(row_copy, j), s)
    for s in (2, 3):
        sent(flat_copy, s)


def per_device(n_row, n_col, fire_state, fuel_class, firebreak, ignition, spread_rate, spread_rows, spread_cols, reaction, ignition_heat):
    c, h, w = fire_state.shape
    k = spread_rate.shape[0]
    k8 = -(-k // 8) * 8
    d = DEPTH
    own, two = h // 2, 2 * c
    total, wide = own + d, w + 2 * d
    groups = total * d // w
    field = pltpu.VMEM((total + 1, wide + 2 * PAD, two), F32)
    terms = pltpu.VMEM((total, wide, two), F32)
    ints = pltpu.VMEM((h + 2 * d, w), jnp.int32)
    dma = pltpu.SemaphoreType.DMA
    out = pl.pallas_call(
        functools.partial(kernel, (n_row, n_col, c, h, w, k8)),
        out_shape=jax.ShapeDtypeStruct((c * h, w), F32),
        in_specs=[pl.BlockSpec(memory_space=pltpu.HBM)] * 9,
        out_specs=pl.BlockSpec(memory_space=pltpu.VMEM),
        scratch_shapes=[
            pltpu.VMEM((c * h, w), F32),
            ints, ints, ints,
            pltpu.VMEM(spread_rate.shape, F32),
            pltpu.VMEM((c, c), F32), pltpu.VMEM((c, c), F32), pltpu.VMEM((c, c), F32),
            pltpu.VMEM((1, c), F32),
            dma((9,)),
            field, field, terms, terms, terms,
            pltpu.VMEM((2 * two, 2 * two), BF16),
            pltpu.VMEM((2 * two, 2 * two), BF16),
            pltpu.VMEM((2 * (k8 + 8), 3 * two), F32),
            pltpu.VMEM((2, d, c, w), F32),
            pltpu.VMEM((2, groups, 8, w), F32),
            pltpu.VMEM((2, groups, 8, w), F32),
            dma((d, 2)), dma((d, 2)), dma((3, 2)), dma((3, 2)), dma((2,)), dma((2,)), dma((2,)), dma((2,)),
            dma((d // CHUNK, 2)), dma((d // CHUNK, 2)),
        ],
        compiler_params=pltpu.CompilerParams(collective_id=0, has_side_effects=True, vmem_limit_bytes=56 * 1048576),
    )(
        fire_state, fuel_class, firebreak, ignition,
        spread_rate, spread_rows, spread_cols, reaction, ignition_heat.reshape(1, c),
    )
    return out.reshape(c, h, w)


def solution(mesh):
    grid = P("row", "col")
    field = P(None, "row", "col")
    return jax.shard_map(
        functools.partial(per_device, mesh.shape["row"], mesh.shape["col"]),
        mesh=mesh,
        in_specs=(field, grid, grid, grid, P(), P(), P(), P(), P()),
        out_specs=field,
        check_vma=False,
    )
```

```python
import functools

import jax
import jax.numpy as jnp
from jax import lax
from jax.experimental import pallas as pl
from jax.experimental.pallas import tpu as pltpu
from jax.sharding import PartitionSpec as P

ITERS = 4
DEPTH = 2 * ITERS
PAD = 8
LARGEST = 6
CHUNK = 4
BF16, F32 = jnp.bfloat16, jnp.float32
MESH = pl.DeviceIdType.MESH


def split(x):
    high = x.astype(BF16)
    return high, (x - high.astype(F32)).astype(BF16)


def dot(a, b):
    return jnp.dot(a, b, preferred_element_type=F32)


def lanes(shape):
    return lax.broadcasted_iota(jnp.int32, shape, 1)


def rows_of(shape):
    return lax.broadcasted_iota(jnp.int32, shape, 0)


def on_diagonal(matrix):
    c = matrix.shape[0]
    turned = matrix.T
    wide = jnp.concatenate([turned, turned], axis=1)
    first = lanes(wide.shape) < c
    return jnp.concatenate([jnp.where(first, wide, 0.0), jnp.where(first, 0.0, wide)], axis=0)


def kernel(
    dims,
    x_hbm, fuel_hbm, break_hbm, lit_hbm, rate_hbm, srow_hbm, scol_hbm, react_hbm, heat_hbm,
    out_ref,
    x_ref, fuel_ref, break_ref, lit_ref, rate_ref, srow_ref, scol_ref, react_ref, heat_ref, load_sem,
    v, mid, coef, burn, heat, ws, wa, wc, halo_x, flat_send, flat_recv,
    row_send, row_recv, int_send, int_recv, col_send, col_recv, flat_ssem, flat_rsem, corner_send, corner_recv,
):
    n_row, n_col, c, h, w, k8 = dims
    d = DEPTH
    own = h // 2
    half_rows = own // 2
    total = own + d
    wide = w + 2 * d
    two = 2 * c
    group = w // d
    groups = total // group
    full = h + 2 * d
    r, q = lax.axis_index("row"), lax.axis_index("col")
    partner = ({"row": r - 1}, {"row": r + 1}, {"col": q - 1}, {"col": q + 1})
    has = (r > 0, r < n_row - 1, q > 0, q < n_col - 1)

    def load(n, src, dst):
        return pltpu.make_async_copy(src, dst, load_sem.at[n])

    body = pl.ds(d, h)
    cell_loads = [
        load(0, fuel_hbm, fuel_ref.at[body]), load(1, break_hbm, break_ref.at[body]), load(2, lit_hbm, lit_ref.at[body]),
        load(3, rate_hbm, rate_ref), load(4, heat_hbm, heat_ref),
    ]
    weight_loads = [load(5, srow_hbm, srow_ref), load(6, scol_hbm, scol_ref), load(7, react_hbm, react_ref)]
    field_load = load(8, x_hbm, x_ref.reshape(c, h, w))
    for one in [field_load] + cell_loads + weight_loads:
        one.start()

    for at in (pl.ds(0, d), pl.ds(h + d, d)):
        fuel_ref[at] = jnp.zeros((d, w), jnp.int32)
        lit_ref[at] = jnp.zeros((d, w), jnp.int32)
        break_ref[at] = jnp.ones((d, w), jnp.int32)
    flat_recv[...] = jnp.ones_like(flat_recv)
    halo_x[...] = jnp.zeros_like(halo_x)
    v[:, PAD:PAD + d] = jnp.zeros((total + 1, d, two), F32)
    v[:, PAD + d + w:PAD + wide] = jnp.zeros((total + 1, d, two), F32)

    barrier = pltpu.get_barrier_semaphore()
    for s in range(4):
        @pl.when(has[s])
        def _(s=s):
            pl.semaphore_signal(barrier, inc=1, device_id=partner[s], device_id_type=MESH)

    def remote(src, dst, send_sem, recv_sem, s):
        return pltpu.make_async_remote_copy(
            src_ref=src, dst_ref=dst, send_sem=send_sem, recv_sem=recv_sem, device_id=partner[s], device_id_type=MESH
        )

    def int_copy(n, s):
        src = (fuel_hbm, break_hbm, lit_hbm)[n]
        dst = (fuel_ref, break_ref, lit_ref)[n]
        from_row, to_row = (0, h + d) if s == 0 else (h - d, 0)
        return remote(src.at[pl.ds(from_row, d)], dst.at[pl.ds(to_row, d)], int_send.at[n, s], int_recv.at[n, s], s)

    def row_copy(j, s):
        src, at = (j, d - 1 - j) if s == 0 else (h - 1 - j, d - 1 - j)
        return remote(x_hbm.at[:, src, :], halo_x.at[s, at], row_send.at[j, s], row_recv.at[j, s], s)

    def edge(s, at):
        if s == 2:
            return v.at[at, PAD + d:PAD + 2 * d], v.at[at, PAD + d + w:PAD + wide]
        return v.at[at, PAD + w:PAD + w + d], v.at[at, PAD:PAD + d]

    def col_copy(m, s):
        src, dst = edge(s, pl.ds(d + m * half_rows, half_rows))
        return remote(src, dst, col_send.at[m, s - 2], col_recv.at[m, s - 2], s)

    def corner_copy(j, s):
        src, dst = edge(s, pl.ds(d - CHUNK * (j + 1), CHUNK))
        return remote(src, dst, corner_send.at[j, s - 2], corner_recv.at[j, s - 2], s)

    def flat_copy(late, s):
        at = pl.ds(groups, 1) if late else pl.ds(0, groups)
        src, dst = flat_send.at[s - 2, at], flat_recv.at[s - 2, at]
        return remote(src, dst, flat_ssem.at[late, s - 2], flat_rsem.at[late, s - 2], s)

    def start(make, s):
        @pl.when(has[s])
        def _():
            make(s).start()

    def sent(make, s):
        @pl.when(has[s])
        def _():
            make(s).wait_send()

    def arrived(make, s):
        @pl.when(has[s ^ 1])
        def _():
            make(s).wait_recv()

    n_near = sum(s.astype(jnp.int32) for s in has)
    pl.semaphore_wait(barrier, n_near)
    for s in range(2):
        for n in range(3):
            start(functools.partial(int_copy, n), s)
    for j in range(d):
        for s in range(2):
            start(functools.partial(row_copy, j), s)

    for one in weight_loads:
        one.wait()
    row_hi, row_lo = split(on_diagonal(srow_ref[...]))
    col_hi, col_lo = split(on_diagonal(scol_ref[...]))
    rea_hi, rea_lo = split(on_diagonal(react_ref[...]))
    ws[0:two] = jnp.concatenate([row_hi, row_lo], axis=1)
    ws[two:2 * two] = jnp.concatenate([col_hi, col_lo], axis=1)
    wa[0:two] = jnp.concatenate([rea_hi, rea_lo], axis=1)
    wa[two:2 * two] = jnp.concatenate([rea_hi, jnp.zeros_like(rea_lo)], axis=1)

    for one in cell_loads:
        one.wait()

    lane = lanes((w, 2 * w))
    from_col = lax.rem(lane, d) + jnp.where(lane < w, 0, w - d)
    pick = jnp.where(rows_of((w, 2 * w)) == from_col, 1.0, 0.0).astype(BF16)
    slot = lax.rem(lanes((group, 2 * w)), w) // d
    ups = rows_of((group, 2 * w)) == slot
    downs = (group - 1) - rows_of((group, 2 * w)) == slot

    def flatten(tall, size, blocks):
        spread_out = dot(tall.astype(BF16), pick)
        for to, g in blocks:
            lines = []
            for half in range(2):
                for n in range(3):
                    first = n * size + (g * group if half == 0 else size - (g + 1) * group)
                    piece = jnp.where(ups if half == 0 else downs, spread_out[first:first + group], 0.0)
                    lines.append(jnp.sum(piece, axis=0, keepdims=True))
            lines.append(jnp.zeros((2, 2 * w), F32))
            packed = jnp.concatenate(lines, axis=0)
            flat_send[0, to] = packed[:, :w]
            flat_send[1, to] = packed[:, w:]

    fill = jnp.zeros((d, w), F32)
    early = []
    for ref in (fuel_ref, break_ref, lit_ref):
        early += [fill, ref[d:d + h].astype(F32), fill]
    flatten(jnp.concatenate(early, axis=0), full, [(g, g) for g in range(groups)])
    for s in (2, 3):
        start(functools.partial(flat_copy, 0), s)

    field_load.wait()

    def turn_in(i, carry):
        tall = jnp.concatenate([x_ref[pl.ds(i, c, stride=h), :], x_ref[pl.ds(h - 1 - i, c, stride=h), :]], axis=0)
        v[d + i, PAD + d:PAD + d + w] = tall.T
        return carry

    for m in range(2):
        lax.fori_loop(m * half_rows, (m + 1) * half_rows, turn_in, 0, unroll=half_rows // 2)
        for s in (2, 3):
            start(functools.partial(col_copy, m), s)

    k = rate_ref.shape[0]
    part = k8 + 8
    rates = jnp.concatenate([rate_ref[...], rate_ref[...]], axis=1)
    heats = jnp.concatenate([heat_ref[...], heat_ref[...]], axis=1)
    wc[...] = jnp.zeros_like(wc)
    for s in range(2):
        mine = (lanes((1, two)) < c) if s == 0 else (lanes((1, two)) >= c)
        wc[s * part:s * part + k, 0:two] = jnp.where(mine, rates, 0.0)
        wc[s * part + k8:s * part + k8 + 1, two:2 * two] = jnp.where(mine, 1.0, 0.0)
        wc[s * part + k8 + 1:s * part + k8 + 2, 2 * two:3 * two] = jnp.where(mine, heats, 0.0)
    tables = jnp.concatenate(split(wc[...]), axis=0)
    classes, slots = rows_of((k8, w)).astype(F32), rows_of((8, w))

    def terms_of(pairs):
        parts = []
        for fuel, broken, lit in pairs:
            alive = 1.0 - broken
            parts.append(jnp.where(fuel == classes, alive, 0.0))
            parts.append(jnp.where(slots == 0, alive, jnp.where(slots == 1, alive * lit, 0.0)))
        tall = jnp.concatenate(parts + parts, axis=0)
        return dot(tall.T.astype(BF16), tables)

    def cells(p, carry):
        pairs = []
        for at in (pl.ds(p, 1), pl.ds(full - 1 - p, 1)):
            pairs.append([ref[at, :].astype(F32) for ref in (fuel_ref, break_ref, lit_ref)])
        terms = terms_of(pairs)
        for n, ref in enumerate((coef, burn, heat)):
            ref[p, d:d + w] = terms[:, n * two:(n + 1) * two]
        return carry

    lax.fori_loop(d, total, cells, 0, unroll=4)

    for s in range(2):
        for n in range(3):
            arrived(functools.partial(int_copy, n), s)
    late = []
    for ref in (fuel_ref, break_ref, lit_ref):
        late += [ref[0:group].astype(F32), ref[full - group:full].astype(F32)]
    flatten(jnp.concatenate(late, axis=0), 2 * group, [(groups, 0)])
    for s in (2, 3):
        start(functools.partial(flat_copy, 1), s)
    lax.fori_loop(0, d, cells, 0, unroll=4)

    def edge_cells(blocks):
        for s in (2, 3):
            to = d + w if s == 2 else 0
            for g, source in blocks:
                lines = flat_recv[s - 2, source]
                terms = terms_of([[lines[3 * half + n:3 * half + n + 1] for n in range(3)] for half in range(2)])
                for n, ref in enumerate((coef, burn, heat)):
                    ref[g * group:(g + 1) * group, to:to + d] = terms[:, n * two:(n + 1) * two].reshape(group, d, two)

    for s in (2, 3):
        arrived(functools.partial(flat_copy, 0), s)
    edge_cells([(g, g) for g in range(groups)])
    for m in range(2):
        for s in (2, 3):
            arrived(functools.partial(col_copy, m), s)
            sent(functools.partial(col_copy, m), s)

    def evaluate(p, n, second, top=False):
        cur, target = (mid, v) if second else (v, mid)
        flat = lambda value: value.reshape(n * wide, two)
        inner = slice(PAD, PAD + wide)
        at = pl.ds(p, n)
        x = flat(cur[at, inner])
        above = flat(cur[pl.ds(p - 1, n), inner])
        if top:
            turned = pltpu.roll(cur[p + n - 1, inner], c, axis=1)
            below = jnp.concatenate([flat(cur[at, inner])[wide:], turned], axis=0)
        else:
            below = flat(cur[pl.ds(p + 1, n), inner])
        left = flat(cur[at, PAD - 1:PAD - 1 + wide])
        right = flat(cur[at, PAD + 1:PAD + 1 + wide])
        twice = x + x
        vertical = (above + below) - twice
        horizontal = (left + right) - twice
        coupled = dot(jnp.concatenate([vertical.astype(BF16), horizontal.astype(BF16)], axis=1), ws[...])
        hi, lo = split(jnp.tanh(x))
        burning = dot(jnp.concatenate([hi, lo], axis=1), wa[...])
        mixed = (vertical + horizontal) + (coupled[:, :two] + coupled[:, two:])
        fire = flat(coef[at]) * mixed + flat(burn[at]) * (burning[:, :two] + burning[:, two:])
        fire = (fire + flat(heat[at])) + 0.5 * x
        if second:
            fire = 0.5 * (fire + flat(v[at, inner]))
        target[at, inner] = fire.reshape(n, wide, two)

    def pyramid(k):
        low, count = d + k, own - k
        blocks = -(-count // LARGEST)
        for b in range(blocks):
            begin, end = count * b // blocks, count * (b + 1) // blocks
            evaluate(low + begin, end - begin, k % 2 == 0, top=b == blocks - 1)

    def take_rows(j):
        for m in range(j * CHUNK, (j + 1) * CHUNK):
            for s in range(2):
                arrived(functools.partial(row_copy, m), s)
        for m in range(CHUNK):
            p = d - CHUNK * (j + 1) + m
            v[p, PAD + d:PAD + d + w] = jnp.concatenate([halo_x[1, p], halo_x[0, p]], axis=0).T
        for s in (2, 3):
            start(functools.partial(corner_copy, j), s)

    def zone(j):
        for s in (2, 3):
            sent(functools.partial(corner_copy, j), s)
            arrived(functools.partial(corner_copy, j), s)

        def step(t, carry):
            low = d - CHUNK * (j + 1) + 2 * t
            evaluate(low + 1, CHUNK, False)
            evaluate(low + 2, CHUNK, True)
            return carry

        lax.fori_loop(0, ITERS, step, 0)

    for k in range(1, 5):
        pyramid(k)
    take_rows(0)
    for k in range(5, 9):
        pyramid(k)
    for s in (2, 3):
        arrived(functools.partial(flat_copy, 1), s)
    edge_cells([(0, groups)])
    zone(0)
    take_rows(1)

    def turn_out(i, carry):
        tall = v[d + i, PAD + d:PAD + d + w].T
        out_ref[pl.ds(i, c, stride=h), :] = tall[:c]
        out_ref[pl.ds(h - 1 - i, c, stride=h), :] = tall[c:]
        return carry

    lax.fori_loop(d, own, turn_out, 0, unroll=8)
    zone(1)
    lax.fori_loop(0, d, turn_out, 0, unroll=8)
    for s in range(2):
        for n in range(3):
            sent(functools.partial(int_copy, n), s)
        for j in range(d):
            sent(functools.partial(row_copy, j), s)
    for s in (2, 3):
        for late in range(2):
            sent(functools.partial(flat_copy, late), s)


def per_device(n_row, n_col, fire_state, fuel_class, firebreak, ignition, spread_rate, spread_rows, spread_cols, reaction, ignition_heat):
    c, h, w = fire_state.shape
    k = spread_rate.shape[0]
    k8 = -(-k // 8) * 8
    d = DEPTH
    own, two = h // 2, 2 * c
    total, wide = own + d, w + 2 * d
    groups = total * d // w
    field = pltpu.VMEM((total + 1, wide + 2 * PAD, two), F32)
    terms = pltpu.VMEM((total, wide, two), F32)
    ints = pltpu.VMEM((h + 2 * d, w), jnp.int32)
    dma = pltpu.SemaphoreType.DMA
    out = pl.pallas_call(
        functools.partial(kernel, (n_row, n_col, c, h, w, k8)),
        out_shape=pltpu.VMEM((c * h, w), F32),
        in_specs=[pl.BlockSpec(memory_space=pltpu.HBM)] * 9,
        out_specs=pl.BlockSpec(memory_space=pltpu.VMEM),
        scratch_shapes=[
            pltpu.VMEM((c * h, w), F32),
            ints, ints, ints,
            pltpu.VMEM(spread_rate.shape, F32),
            pltpu.VMEM((c, c), F32), pltpu.VMEM((c, c), F32), pltpu.VMEM((c, c), F32),
            pltpu.VMEM((1, c), F32),
            dma((9,)),
            field, field, terms, terms, terms,
            pltpu.VMEM((2 * two, 2 * two), BF16),
            pltpu.VMEM((2 * two, 2 * two), BF16),
            pltpu.VMEM((2 * (k8 + 8), 3 * two), F32),
            pltpu.VMEM((2, d, c, w), F32),
            pltpu.VMEM((2, groups + 1, 8, w), F32),
            pltpu.VMEM((2, groups + 1, 8, w), F32),
            dma((d, 2)), dma((d, 2)), dma((3, 2)), dma((3, 2)), dma((2, 2)), dma((2, 2)), dma((2, 2)), dma((2, 2)),
            dma((d // CHUNK, 2)), dma((d // CHUNK, 2)),
        ],
        compiler_params=pltpu.CompilerParams(collective_id=0, has_side_effects=True, vmem_limit_bytes=56 * 1048576),
    )(
        fire_state, fuel_class, firebreak, ignition,
        spread_rate, spread_rows, spread_cols, reaction, ignition_heat.reshape(1, c),
    )
    return out.reshape(c, h, w)


def solution(mesh):
    grid = P("row", "col")
    field = P(None, "row", "col")
    return jax.shard_map(
        functools.partial(per_device, mesh.shape["row"], mesh.shape["col"]),
        mesh=mesh,
        in_specs=(field, grid, grid, grid, P(), P(), P(), P(), P()),
        out_specs=field,
        check_vma=False,
    )
```

```python
import functools

import jax
import jax.numpy as jnp
from jax import lax
from jax.experimental import pallas as pl
from jax.experimental.pallas import tpu as pltpu
from jax.sharding import PartitionSpec as P

ITERS = 4
DEPTH = 2 * ITERS
PAD = 8
TILE = 8
LARGEST = 72
EARLY = 3
CHUNK = 4
BF16, F32 = jnp.bfloat16, jnp.float32
ROUND = 1.5 * 2.0 ** 15
MESH = pl.DeviceIdType.MESH


def split(x):
    high = x.astype(BF16)
    return high, (x - high.astype(F32)).astype(BF16)


def dot(a, b):
    return jnp.dot(a, b, preferred_element_type=F32)


def mixed_dot(a, b):
    return lax.dot_general(a, b, (((1,), (0,)), ((), ())), preferred_element_type=F32)


def lanes(shape):
    return lax.broadcasted_iota(jnp.int32, shape, 1)


def rows_of(shape):
    return lax.broadcasted_iota(jnp.int32, shape, 0)


def on_diagonal(matrix):
    c = matrix.shape[0]
    turned = matrix.T
    wide = jnp.concatenate([turned, turned], axis=1)
    first = lanes(wide.shape) < c
    return jnp.concatenate([jnp.where(first, wide, 0.0), jnp.where(first, 0.0, wide)], axis=0)


def kernel(
    dims,
    x_hbm, fuel_hbm, break_hbm, lit_hbm, rate_hbm, srow_hbm, scol_hbm, react_hbm, heat_hbm,
    out_ref,
    x_ref, fuel_ref, break_ref, lit_ref, rate_ref, srow_ref, scol_ref, react_ref, heat_ref, load_sem,
    v, mid, coef, burn, heat, ws, wa, wc, halo_x, relay_x, flat_send, flat_recv,
    row_send, row_recv, int_send, int_recv, col_send, col_recv, flat_ssem, flat_rsem, corner_send, corner_recv,
    relay_send, relay_recv,
):
    n_row, n_col, c, h, w, k8 = dims
    d = DEPTH
    own = h // 2
    total = own + d
    wide = w + 2 * d
    two = 2 * c
    group = w // d
    groups = total // group
    full = h + 2 * d
    r, q = lax.axis_index("row"), lax.axis_index("col")
    odd = lax.rem(r, 2) == 1
    partner = ({"row": r - 1}, {"row": r + 1}, {"col": q - 1}, {"col": q + 1}, {"row": r - 2}, {"row": r + 2})
    has = (r > 0, r < n_row - 1, q > 0, q < n_col - 1, r > 1, r < n_row - 2)

    def load(n, src, dst):
        return pltpu.make_async_copy(src, dst, load_sem.at[n])

    body = pl.ds(d, h)
    cell_loads = [
        load(0, fuel_hbm, fuel_ref.at[body]), load(1, break_hbm, break_ref.at[body]), load(2, lit_hbm, lit_ref.at[body]),
        load(3, rate_hbm, rate_ref), load(4, heat_hbm, heat_ref),
    ]
    weight_loads = [load(5, srow_hbm, srow_ref), load(6, scol_hbm, scol_ref), load(7, react_hbm, react_ref)]
    x_rows = x_ref.reshape(c, h, w)
    field_load = load(8, x_hbm, x_rows)
    for one in [field_load] + cell_loads + weight_loads:
        one.start()

    for at in (pl.ds(0, d), pl.ds(h + d, d)):
        fuel_ref[at] = jnp.zeros((d, w), jnp.int32)
        lit_ref[at] = jnp.zeros((d, w), jnp.int32)
        break_ref[at] = jnp.ones((d, w), jnp.int32)
    flat_recv[...] = jnp.ones_like(flat_recv)
    halo_x[...] = jnp.zeros_like(halo_x)
    v[:, PAD:PAD + d] = jnp.zeros((total + 1, d, two), F32)
    v[:, PAD + d + w:PAD + wide] = jnp.zeros((total + 1, d, two), F32)

    barrier = pltpu.get_barrier_semaphore()
    for s in range(6):
        @pl.when(has[s])
        def _(s=s):
            pl.semaphore_signal(barrier, inc=1, device_id=partner[s], device_id_type=MESH)

    def remote(src, dst, send_sem, recv_sem, s):
        return pltpu.make_async_remote_copy(
            src_ref=src, dst_ref=dst, send_sem=send_sem, recv_sem=recv_sem, device_id=partner[s], device_id_type=MESH
        )

    def int_copy(n, s):
        src = (fuel_hbm, break_hbm, lit_hbm)[n]
        dst = (fuel_ref, break_ref, lit_ref)[n]
        from_row, to_row = (0, h + d) if s == 0 else (h - d, 0)
        return remote(src.at[pl.ds(from_row, d)], dst.at[pl.ds(to_row, d)], int_send.at[n, s], int_recv.at[n, s], s)

    def row_copy(j, s):
        src, at = (j, d - 1 - j) if s == 0 else (h - 1 - j, d - 1 - j)
        return remote(x_hbm.at[:, src, :], halo_x.at[s, at], row_send.at[j, s], row_recv.at[j, s], s)

    detour = (jnp.logical_and(jnp.logical_not(odd), has[4]), jnp.logical_and(odd, has[5]))
    relays = (jnp.logical_and(jnp.logical_not(odd), has[5]), jnp.logical_and(odd, has[4]))

    def detour_copy(j, s):
        src = j if s == 0 else h - 1 - j
        at = j - CHUNK
        return remote(x_hbm.at[:, src, :], relay_x.at[at], row_send.at[j, s], relay_recv.at[at], s + 4)

    def relay_copy(j, s):
        at = j - CHUNK
        return remote(relay_x.at[at], halo_x.at[s, d - 1 - j], relay_send.at[at], row_recv.at[j, s], 1 - s)

    def start_far(j, s):
        @pl.when(jnp.logical_and(has[s], jnp.logical_not(detour[s])))
        def _():
            row_copy(j, s).start()

        @pl.when(detour[s])
        def _():
            detour_copy(j, s).start()

    def relay():
        for s in range(2):
            @pl.when(relays[s])
            def _(s=s):
                for j in range(CHUNK, d):
                    detour_copy(j, s).wait_recv()
                    relay_copy(j, s).start()

    def relayed():
        for s in range(2):
            @pl.when(relays[s])
            def _(s=s):
                for j in range(CHUNK, d):
                    relay_copy(j, s).wait_send()

    def edge(s, at):
        if s == 2:
            return v.at[at, PAD + d:PAD + 2 * d], v.at[at, PAD + d + w:PAD + wide]
        return v.at[at, PAD + w:PAD + w + d], v.at[at, PAD:PAD + d]

    def col_copy(m, s):
        src, dst = edge(s, pl.ds(d + m * TILE, TILE))
        return remote(src, dst, col_send.at[m, s - 2], col_recv.at[m, s - 2], s)

    def corner_copy(j, s):
        src, dst = edge(s, pl.ds(d - CHUNK * (j + 1), CHUNK))
        return remote(src, dst, corner_send.at[j, s - 2], corner_recv.at[j, s - 2], s)

    def flat_copy(late, s):
        at = pl.ds(groups, 1) if late else pl.ds(0, groups)
        src, dst = flat_send.at[s - 2, at], flat_recv.at[s - 2, at]
        return remote(src, dst, flat_ssem.at[late, s - 2], flat_rsem.at[late, s - 2], s)

    def start(make, s):
        @pl.when(has[s])
        def _():
            make(s).start()

    def sent(make, s):
        @pl.when(has[s])
        def _():
            make(s).wait_send()

    def arrived(make, s):
        @pl.when(has[s ^ 1])
        def _():
            make(s).wait_recv()

    n_near = sum(s.astype(jnp.int32) for s in has)
    pl.semaphore_wait(barrier, n_near)
    for s in range(2):
        for n in range(3):
            start(functools.partial(int_copy, n), s)
    for j in range(d):
        for s in range(2):
            if j < CHUNK:
                start(functools.partial(row_copy, j), s)
            else:
                start_far(j, s)

    field_load.wait()
    for m in range(own // TILE):
        for i in range(m * TILE, (m + 1) * TILE):
            tall = jnp.concatenate([x_ref[pl.ds(i, c, stride=h), :], x_ref[pl.ds(h - 1 - i, c, stride=h), :]], axis=0)
            v[d + i, PAD + d:PAD + d + w] = tall.T
        for s in (2, 3):
            start(functools.partial(col_copy, m), s)

    for one in weight_loads:
        one.wait()
    row_hi, row_lo = split(on_diagonal(srow_ref[...]))
    col_hi, col_lo = split(on_diagonal(scol_ref[...]))
    rea_hi, rea_lo = split(on_diagonal(react_ref[...]))
    ws[0:two] = jnp.concatenate([row_hi, row_lo], axis=1)
    ws[two:2 * two] = jnp.concatenate([col_hi, col_lo], axis=1)
    wa[0:two] = jnp.concatenate([rea_hi, rea_lo], axis=1)
    wa[two:2 * two] = jnp.concatenate([rea_hi, jnp.zeros_like(rea_lo)], axis=1)

    for one in cell_loads:
        one.wait()

    lane = lanes((w, 2 * w))
    from_col = lax.rem(lane, d) + jnp.where(lane < w, 0, w - d)
    pick = jnp.where(rows_of((w, 2 * w)) == from_col, 1.0, 0.0).astype(BF16)
    slot = lax.rem(lanes((group, 2 * w)), w) // d
    ups = rows_of((group, 2 * w)) == slot
    downs = (group - 1) - rows_of((group, 2 * w)) == slot

    def flatten(tall, size, blocks):
        spread_out = dot(tall.astype(BF16), pick)
        for to, g in blocks:
            lines = []
            for half in range(2):
                for n in range(3):
                    first = n * size + (g * group if half == 0 else size - (g + 1) * group)
                    piece = jnp.where(ups if half == 0 else downs, spread_out[first:first + group], 0.0)
                    lines.append(jnp.sum(piece, axis=0, keepdims=True))
            lines.append(jnp.zeros((2, 2 * w), F32))
            packed = jnp.concatenate(lines, axis=0)
            flat_send[0, to] = packed[:, :w]
            flat_send[1, to] = packed[:, w:]

    fill = jnp.zeros((d, w), F32)
    early = []
    for ref in (fuel_ref, break_ref, lit_ref):
        early += [fill, ref[d:d + h].astype(F32), fill]
    flatten(jnp.concatenate(early, axis=0), full, [(g, g) for g in range(groups)])
    for s in (2, 3):
        start(functools.partial(flat_copy, 0), s)

    k = rate_ref.shape[0]
    part = k8 + 8
    rates = jnp.concatenate([rate_ref[...], rate_ref[...]], axis=1)
    heats = jnp.concatenate([heat_ref[...], heat_ref[...]], axis=1)
    wc[...] = jnp.zeros_like(wc)
    for s in range(2):
        mine = (lanes((1, two)) < c) if s == 0 else (lanes((1, two)) >= c)
        wc[s * part:s * part + k, 0:two] = jnp.where(mine, rates, 0.0)
        wc[s * part + k8:s * part + k8 + 1, two:2 * two] = jnp.where(mine, 1.0, 0.0)
        wc[s * part + k8 + 1:s * part + k8 + 2, 2 * two:3 * two] = jnp.where(mine, heats, 0.0)
    tables = jnp.concatenate(split(wc[...]), axis=0)
    classes, slots = rows_of((k8, w)).astype(F32), rows_of((8, w))

    def terms_of(pairs):
        parts = []
        for fuel, broken, lit in pairs:
            alive = 1.0 - broken
            parts.append(jnp.where(fuel == classes, alive, 0.0))
            parts.append(jnp.where(slots == 0, alive, jnp.where(slots == 1, alive * lit, 0.0)))
        tall = jnp.concatenate(parts + parts, axis=0)
        return dot(tall.T.astype(BF16), tables)

    def cells(p, carry):
        pairs = []
        for at in (pl.ds(p, 1), pl.ds(full - 1 - p, 1)):
            pairs.append([ref[at, :].astype(F32) for ref in (fuel_ref, break_ref, lit_ref)])
        terms = terms_of(pairs)
        for n, ref in enumerate((coef, burn, heat)):
            ref[p, d:d + w] = terms[:, n * two:(n + 1) * two]
        return carry

    lax.fori_loop(d, total, cells, 0, unroll=4)

    def edge_cells(blocks):
        for s in (2, 3):
            to = d + w if s == 2 else 0
            for g, source in blocks:
                lines = flat_recv[s - 2, source]
                terms = terms_of([[lines[3 * half + n:3 * half + n + 1] for n in range(3)] for half in range(2)])
                for n, ref in enumerate((coef, burn, heat)):
                    ref[g * group:(g + 1) * group, to:to + d] = terms[:, n * two:(n + 1) * two].reshape(group, d, two)

    def take_cols():
        for s in (2, 3):
            arrived(functools.partial(flat_copy, 0), s)
        edge_cells([(g, g) for g in range(groups)])
        for m in range(own // TILE):
            for s in (2, 3):
                arrived(functools.partial(col_copy, m), s)

    tiles = wide // TILE

    def evaluate(p, n, second, first=0, last=tiles, top=False):
        cur, target = (mid, v) if second else (v, mid)
        size = (last - first) * TILE
        flat = lambda value: value.reshape(n * size, two)
        side = lambda shift: slice(PAD + first * TILE + shift, PAD + last * TILE + shift)
        inner, cell = side(0), side(-PAD)
        at = pl.ds(p, n)
        x = flat(cur[at, inner])
        above = flat(cur[pl.ds(p - 1, n), inner])
        if top:
            turned = pltpu.roll(cur[p + n - 1, inner], c, axis=1)
            below = jnp.concatenate([x[size:], turned], axis=0) if n > 1 else turned
        else:
            below = flat(cur[pl.ds(p + 1, n), inner])
        left, right = flat(cur[at, side(-1)]), flat(cur[at, side(1)])
        twice = x + x
        vertical = (above + below) - twice
        horizontal = (left + right) - twice
        coupled = mixed_dot(jnp.concatenate([vertical, horizontal], axis=1), ws[...])
        burnt = jnp.tanh(x)
        hi = (burnt + ROUND) - ROUND
        burning = mixed_dot(jnp.concatenate([hi, burnt - hi], axis=1), wa[...])
        mixed = (vertical + horizontal) + (coupled[:, :two] + coupled[:, two:])
        fire = flat(coef[at, cell]) * mixed + flat(burn[at, cell]) * (burning[:, :two] + burning[:, two:])
        fire = (fire + flat(heat[at, cell])) + 0.5 * x
        if second:
            fire = 0.5 * (fire + flat(v[at, inner]))
        target[at, inner] = fire.reshape(n, size, two)

    def pyramid(k, first=0, last=tiles):
        if k == d:
            first, last = max(first, 1), min(last, tiles - 1)
        low, count = d + k, own - k
        blocks = -(-count * (last - first) // LARGEST)
        for b in range(blocks):
            begin, end = count * b // blocks, count * (b + 1) // blocks
            evaluate(low + begin, end - begin, k % 2 == 0, first, last, top=b == blocks - 1)

    def take_ints():
        for s in range(2):
            for n in range(3):
                arrived(functools.partial(int_copy, n), s)
        late = []
        for ref in (fuel_ref, break_ref, lit_ref):
            late += [ref[0:group].astype(F32), ref[full - group:full].astype(F32)]
        flatten(jnp.concatenate(late, axis=0), 2 * group, [(groups, 0)])
        for s in (2, 3):
            start(functools.partial(flat_copy, 1), s)
        lax.fori_loop(0, d, cells, 0, unroll=4)

    def take_rows(j):
        for m in range(j * CHUNK, (j + 1) * CHUNK):
            for s in range(2):
                arrived(functools.partial(row_copy, m), s)
        for m in range(CHUNK):
            p = d - CHUNK * (j + 1) + m
            v[p, PAD + d:PAD + d + w] = jnp.concatenate([halo_x[1, p], halo_x[0, p]], axis=0).T
        for s in (2, 3):
            start(functools.partial(corner_copy, j), s)

    def turn_out(i):
        tall = v[d + i, PAD + d:PAD + d + w].T
        out_ref[pl.ds(i, c, stride=h), :] = tall[:c]
        out_ref[pl.ds(h - 1 - i, c, stride=h), :] = tall[c:]

    def zone(j):
        for s in (2, 3):
            sent(functools.partial(corner_copy, j), s)
            arrived(functools.partial(corner_copy, j), s)
        if j == 1:
            for i in range(d, own):
                turn_out(i)

        for k in range(1, d + 1):
            edge_tile = 1 if k == d else 0
            evaluate(d - CHUNK * (j + 1) + k, CHUNK, k % 2 == 0, edge_tile, tiles - edge_tile)

    for k in range(1, EARLY + 1):
        pyramid(k, k + 1, tiles - k - 1)
    take_cols()
    relay()
    for m in range(own // TILE):
        for s in (2, 3):
            sent(functools.partial(col_copy, m), s)
    for k in range(1, EARLY + 1):
        pyramid(k, 0, k + 1)
        pyramid(k, tiles - k - 1, tiles)
    take_ints()
    take_rows(0)
    for k in range(EARLY + 1, d + 1):
        pyramid(k)
    take_rows(1)
    for s in (2, 3):
        arrived(functools.partial(flat_copy, 1), s)
    edge_cells([(0, groups)])
    zone(0)

    zone(1)
    for i in range(d):
        turn_out(i)
    for s in range(2):
        for n in range(3):
            sent(functools.partial(int_copy, n), s)
        for j in range(d):
            sent(functools.partial(row_copy, j), s)
    for s in (2, 3):
        for late in range(2):
            sent(functools.partial(flat_copy, late), s)
    relayed()


def per_device(n_row, n_col, fire_state, fuel_class, firebreak, ignition, spread_rate, spread_rows, spread_cols, reaction, ignition_heat):
    c, h, w = fire_state.shape
    k = spread_rate.shape[0]
    k8 = -(-k // 8) * 8
    d = DEPTH
    own, two = h // 2, 2 * c
    total, wide = own + d, w + 2 * d
    groups = total * d // w
    field = pltpu.VMEM((total + 1, wide + 2 * PAD, two), F32)
    terms = pltpu.VMEM((total, wide, two), F32)
    ints = pltpu.VMEM((h + 2 * d, w), jnp.int32)
    dma = pltpu.SemaphoreType.DMA
    out = pl.pallas_call(
        functools.partial(kernel, (n_row, n_col, c, h, w, k8)),
        out_shape=pltpu.VMEM((c * h, w), F32),
        in_specs=[pl.BlockSpec(memory_space=pltpu.HBM)] * 9,
        out_specs=pl.BlockSpec(memory_space=pltpu.VMEM),
        scratch_shapes=[
            pltpu.VMEM((c * h, w), F32),
            ints, ints, ints,
            pltpu.VMEM(spread_rate.shape, F32),
            pltpu.VMEM((c, c), F32), pltpu.VMEM((c, c), F32), pltpu.VMEM((c, c), F32),
            pltpu.VMEM((1, c), F32),
            dma((9,)),
            field, field, terms, terms, terms,
            pltpu.VMEM((2 * two, 2 * two), BF16),
            pltpu.VMEM((2 * two, 2 * two), BF16),
            pltpu.VMEM((2 * (k8 + 8), 3 * two), F32),
            pltpu.VMEM((2, d, c, w), F32),
            pltpu.VMEM((d - CHUNK, c, w), F32),
            pltpu.VMEM((2, groups + 1, 8, w), F32),
            pltpu.VMEM((2, groups + 1, 8, w), F32),
            dma((d, 2)), dma((d, 2)), dma((3, 2)), dma((3, 2)), dma((own // TILE, 2)), dma((own // TILE, 2)), dma((2, 2)), dma((2, 2)),
            dma((d // CHUNK, 2)), dma((d // CHUNK, 2)),
            dma((d - CHUNK,)), dma((d - CHUNK,)),
        ],
        compiler_params=pltpu.CompilerParams(collective_id=0, has_side_effects=True, vmem_limit_bytes=56 * 1048576),
    )(
        fire_state, fuel_class, firebreak, ignition,
        spread_rate, spread_rows, spread_cols, reaction, ignition_heat.reshape(1, c),
    )
    return out.reshape(c, h, w)


def solution(mesh):
    grid = P("row", "col")
    field = P(None, "row", "col")
    return jax.shard_map(
        functools.partial(per_device, mesh.shape["row"], mesh.shape["col"]),
        mesh=mesh,
        in_specs=(field, grid, grid, grid, P(), P(), P(), P(), P()),
        out_specs=field,
        check_vma=False,
    )
```

```python
import functools

import jax
import jax.numpy as jnp
from jax import lax
from jax.experimental import pallas as pl
from jax.experimental.pallas import tpu as pltpu
from jax.sharding import PartitionSpec as P

ITERS = 4
DEPTH = 2 * ITERS
PAD = 8
TILE = 8
LARGEST = 72
EARLY = 4
CHUNK = 4
BF16, F32 = jnp.bfloat16, jnp.float32
ROUND = 1.5 * 2.0 ** 15
MESH = pl.DeviceIdType.MESH


def split(x):
    high = x.astype(BF16)
    return high, (x - high.astype(F32)).astype(BF16)


def dot(a, b):
    return jnp.dot(a, b, preferred_element_type=F32)


def mixed_dot(a, b):
    return lax.dot_general(a, b, (((1,), (0,)), ((), ())), preferred_element_type=F32)


def lanes(shape):
    return lax.broadcasted_iota(jnp.int32, shape, 1)


def rows_of(shape):
    return lax.broadcasted_iota(jnp.int32, shape, 0)


def on_diagonal(matrix):
    c = matrix.shape[0]
    turned = matrix.T
    wide = jnp.concatenate([turned, turned], axis=1)
    first = lanes(wide.shape) < c
    return jnp.concatenate([jnp.where(first, wide, 0.0), jnp.where(first, 0.0, wide)], axis=0)


def kernel(
    dims,
    x_hbm, fuel_hbm, break_hbm, lit_hbm, rate_hbm, srow_hbm, scol_hbm, react_hbm, heat_hbm,
    out_ref,
    x_ref, fuel_ref, break_ref, lit_ref, rate_ref, srow_ref, scol_ref, react_ref, heat_ref, load_sem,
    v, mid, coef, burn, heat, ws, wa, wc, halo_x, relay_x, flat_send, flat_recv,
    row_send, row_recv, int_send, int_recv, col_send, col_recv, flat_ssem, flat_rsem, corner_send, corner_recv,
    relay_send, relay_recv,
):
    n_row, n_col, c, h, w, k8 = dims
    d = DEPTH
    own = h // 2
    total = own + d
    wide = w + 2 * d
    two = 2 * c
    group = w // d
    groups = total // group
    full = h + 2 * d
    r, q = lax.axis_index("row"), lax.axis_index("col")
    odd = lax.rem(r, 2) == 1
    partner = ({"row": r - 1}, {"row": r + 1}, {"col": q - 1}, {"col": q + 1}, {"row": r - 2}, {"row": r + 2})
    has = (r > 0, r < n_row - 1, q > 0, q < n_col - 1, r > 1, r < n_row - 2)

    def load(n, src, dst):
        return pltpu.make_async_copy(src, dst, load_sem.at[n])

    body = pl.ds(d, h)
    cell_loads = [
        load(0, fuel_hbm, fuel_ref.at[body]), load(1, break_hbm, break_ref.at[body]), load(2, lit_hbm, lit_ref.at[body]),
        load(3, rate_hbm, rate_ref), load(4, heat_hbm, heat_ref),
    ]
    weight_loads = [load(5, srow_hbm, srow_ref), load(6, scol_hbm, scol_ref), load(7, react_hbm, react_ref)]
    x_rows = x_ref.reshape(c, h, w)
    field_load = load(8, x_hbm, x_rows)
    for one in [field_load] + cell_loads + weight_loads:
        one.start()

    for at in (pl.ds(0, d), pl.ds(h + d, d)):
        fuel_ref[at] = jnp.zeros((d, w), jnp.int32)
        lit_ref[at] = jnp.zeros((d, w), jnp.int32)
        break_ref[at] = jnp.ones((d, w), jnp.int32)
    flat_recv[...] = jnp.ones_like(flat_recv)
    halo_x[...] = jnp.zeros_like(halo_x)
    v[:, PAD:PAD + d] = jnp.zeros((total + 1, d, two), F32)
    v[:, PAD + d + w:PAD + wide] = jnp.zeros((total + 1, d, two), F32)

    barrier = pltpu.get_barrier_semaphore()
    for s in range(6):
        @pl.when(has[s])
        def _(s=s):
            pl.semaphore_signal(barrier, inc=1, device_id=partner[s], device_id_type=MESH)

    def remote(src, dst, send_sem, recv_sem, s):
        return pltpu.make_async_remote_copy(
            src_ref=src, dst_ref=dst, send_sem=send_sem, recv_sem=recv_sem, device_id=partner[s], device_id_type=MESH
        )

    def int_copy(n, s):
        src = (fuel_hbm, break_hbm, lit_hbm)[n]
        dst = (fuel_ref, break_ref, lit_ref)[n]
        from_row, to_row = (0, h + d) if s == 0 else (h - d, 0)
        return remote(src.at[pl.ds(from_row, d)], dst.at[pl.ds(to_row, d)], int_send.at[n, s], int_recv.at[n, s], s)

    def row_copy(j, s):
        src, at = (j, d - 1 - j) if s == 0 else (h - 1 - j, d - 1 - j)
        return remote(x_hbm.at[:, src, :], halo_x.at[s, at], row_send.at[j, s], row_recv.at[j, s], s)

    detour = (jnp.logical_and(jnp.logical_not(odd), has[4]), jnp.logical_and(odd, has[5]))
    relays = (jnp.logical_and(jnp.logical_not(odd), has[5]), jnp.logical_and(odd, has[4]))

    def detour_copy(j, s):
        src = j if s == 0 else h - 1 - j
        at = j - CHUNK
        return remote(x_hbm.at[:, src, :], relay_x.at[at], row_send.at[j, s], relay_recv.at[at], s + 4)

    def relay_copy(j, s):
        at = j - CHUNK
        return remote(relay_x.at[at], halo_x.at[s, d - 1 - j], relay_send.at[at], row_recv.at[j, s], 1 - s)

    def start_far(j, s):
        @pl.when(jnp.logical_and(has[s], jnp.logical_not(detour[s])))
        def _():
            row_copy(j, s).start()

        @pl.when(detour[s])
        def _():
            detour_copy(j, s).start()

    def relay():
        for s in range(2):
            @pl.when(relays[s])
            def _(s=s):
                for j in range(CHUNK, d):
                    detour_copy(j, s).wait_recv()
                    relay_copy(j, s).start()

    def relayed():
        for s in range(2):
            @pl.when(relays[s])
            def _(s=s):
                for j in range(CHUNK, d):
                    relay_copy(j, s).wait_send()

    def edge(s, at):
        if s == 2:
            return v.at[at, PAD + d:PAD + 2 * d], v.at[at, PAD + d + w:PAD + wide]
        return v.at[at, PAD + w:PAD + w + d], v.at[at, PAD:PAD + d]

    def col_copy(m, s):
        src, dst = edge(s, pl.ds(d + m * TILE, TILE))
        return remote(src, dst, col_send.at[m, s - 2], col_recv.at[m, s - 2], s)

    def corner_copy(j, s):
        src, dst = edge(s, pl.ds(d - CHUNK * (j + 1), CHUNK))
        return remote(src, dst, corner_send.at[j, s - 2], corner_recv.at[j, s - 2], s)

    def flat_copy(late, s):
        at = pl.ds(groups, 1) if late else pl.ds(0, groups)
        src, dst = flat_send.at[s - 2, at], flat_recv.at[s - 2, at]
        return remote(src, dst, flat_ssem.at[late, s - 2], flat_rsem.at[late, s - 2], s)

    def start(make, s):
        @pl.when(has[s])
        def _():
            make(s).start()

    def sent(make, s):
        @pl.when(has[s])
        def _():
            make(s).wait_send()

    def arrived(make, s):
        @pl.when(has[s ^ 1])
        def _():
            make(s).wait_recv()

    n_near = sum(s.astype(jnp.int32) for s in has)
    pl.semaphore_wait(barrier, n_near)
    for s in range(2):
        for n in range(3):
            start(functools.partial(int_copy, n), s)
    for j in range(d):
        for s in range(2):
            if j < CHUNK:
                start(functools.partial(row_copy, j), s)
            else:
                start_far(j, s)

    field_load.wait()
    for m in range(own // TILE):
        for i in range(m * TILE, (m + 1) * TILE):
            tall = jnp.concatenate([x_ref[pl.ds(i, c, stride=h), :], x_ref[pl.ds(h - 1 - i, c, stride=h), :]], axis=0)
            v[d + i, PAD + d:PAD + d + w] = tall.T
        for s in (2, 3):
            start(functools.partial(col_copy, m), s)

    for one in weight_loads:
        one.wait()
    row_hi, row_lo = split(on_diagonal(srow_ref[...]))
    col_hi, col_lo = split(on_diagonal(scol_ref[...]))
    rea_hi, rea_lo = split(on_diagonal(react_ref[...]))
    ws[0:two] = jnp.concatenate([row_hi, row_lo], axis=1)
    ws[two:2 * two] = jnp.concatenate([col_hi, col_lo], axis=1)
    wa[0:two] = jnp.concatenate([rea_hi, rea_lo], axis=1)
    wa[two:2 * two] = jnp.concatenate([rea_hi, jnp.zeros_like(rea_lo)], axis=1)

    for one in cell_loads:
        one.wait()

    lane = lanes((w, 2 * w))
    from_col = lax.rem(lane, d) + jnp.where(lane < w, 0, w - d)
    pick = jnp.where(rows_of((w, 2 * w)) == from_col, 1.0, 0.0).astype(BF16)
    slot = lax.rem(lanes((group, 2 * w)), w) // d
    ups = rows_of((group, 2 * w)) == slot
    downs = (group - 1) - rows_of((group, 2 * w)) == slot

    def flatten(tall, size, blocks):
        spread_out = dot(tall.astype(BF16), pick)
        for to, g in blocks:
            lines = []
            for half in range(2):
                for n in range(3):
                    first = n * size + (g * group if half == 0 else size - (g + 1) * group)
                    piece = jnp.where(ups if half == 0 else downs, spread_out[first:first + group], 0.0)
                    lines.append(jnp.sum(piece, axis=0, keepdims=True))
            lines.append(jnp.zeros((2, 2 * w), F32))
            packed = jnp.concatenate(lines, axis=0)
            flat_send[0, to] = packed[:, :w]
            flat_send[1, to] = packed[:, w:]

    fill = jnp.zeros((d, w), F32)
    early = []
    for ref in (fuel_ref, break_ref, lit_ref):
        early += [fill, ref[d:d + h].astype(F32), fill]
    flatten(jnp.concatenate(early, axis=0), full, [(g, g) for g in range(groups)])
    for s in (2, 3):
        start(functools.partial(flat_copy, 0), s)

    k = rate_ref.shape[0]
    part = k8 + 8
    rates = jnp.concatenate([rate_ref[...], rate_ref[...]], axis=1)
    heats = jnp.concatenate([heat_ref[...], heat_ref[...]], axis=1)
    wc[...] = jnp.zeros_like(wc)
    for s in range(2):
        mine = (lanes((1, two)) < c) if s == 0 else (lanes((1, two)) >= c)
        wc[s * part:s * part + k, 0:two] = jnp.where(mine, rates, 0.0)
        wc[s * part + k8:s * part + k8 + 1, two:2 * two] = jnp.where(mine, 1.0, 0.0)
        wc[s * part + k8 + 1:s * part + k8 + 2, 2 * two:3 * two] = jnp.where(mine, heats, 0.0)
    tables = jnp.concatenate(split(wc[...]), axis=0)
    classes, slots = rows_of((k8, w)).astype(F32), rows_of((8, w))

    def terms_of(pairs):
        parts = []
        for fuel, broken, lit in pairs:
            alive = 1.0 - broken
            parts.append(jnp.where(fuel == classes, alive, 0.0))
            parts.append(jnp.where(slots == 0, alive, jnp.where(slots == 1, alive * lit, 0.0)))
        tall = jnp.concatenate(parts + parts, axis=0)
        return dot(tall.T.astype(BF16), tables)

    def cells(p, carry):
        pairs = []
        for at in (pl.ds(p, 1), pl.ds(full - 1 - p, 1)):
            pairs.append([ref[at, :].astype(F32) for ref in (fuel_ref, break_ref, lit_ref)])
        terms = terms_of(pairs)
        for n, ref in enumerate((coef, burn, heat)):
            ref[p, d:d + w] = terms[:, n * two:(n + 1) * two]
        return carry

    lax.fori_loop(d, total, cells, 0, unroll=4)

    def edge_cells(blocks):
        for s in (2, 3):
            to = d + w if s == 2 else 0
            for g, source in blocks:
                lines = flat_recv[s - 2, source]
                terms = terms_of([[lines[3 * half + n:3 * half + n + 1] for n in range(3)] for half in range(2)])
                for n, ref in enumerate((coef, burn, heat)):
                    ref[g * group:(g + 1) * group, to:to + d] = terms[:, n * two:(n + 1) * two].reshape(group, d, two)

    def take_cols():
        for s in (2, 3):
            arrived(functools.partial(flat_copy, 0), s)
        edge_cells([(g, g) for g in range(groups)])
        for m in range(own // TILE):
            for s in (2, 3):
                arrived(functools.partial(col_copy, m), s)

    tiles = wide // TILE

    def evaluate(p, n, second, first=0, last=tiles, top=False):
        cur, target = (mid, v) if second else (v, mid)
        size = (last - first) * TILE
        flat = lambda value: value.reshape(n * size, two)
        side = lambda shift: slice(PAD + first * TILE + shift, PAD + last * TILE + shift)
        inner, cell = side(0), side(-PAD)
        at = pl.ds(p, n)
        x = flat(cur[at, inner])
        above = flat(cur[pl.ds(p - 1, n), inner])
        if top:
            turned = pltpu.roll(cur[p + n - 1, inner], c, axis=1)
            below = jnp.concatenate([x[size:], turned], axis=0) if n > 1 else turned
        else:
            below = flat(cur[pl.ds(p + 1, n), inner])
        left, right = flat(cur[at, side(-1)]), flat(cur[at, side(1)])
        twice = x + x
        vertical = (above + below) - twice
        horizontal = (left + right) - twice
        coupled = mixed_dot(jnp.concatenate([vertical, horizontal], axis=1), ws[...])
        burnt = jnp.tanh(x)
        hi = (burnt + ROUND) - ROUND
        burning = mixed_dot(jnp.concatenate([hi, burnt - hi], axis=1), wa[...])
        mixed = (vertical + horizontal) + (coupled[:, :two] + coupled[:, two:])
        fire = flat(coef[at, cell]) * mixed + flat(burn[at, cell]) * (burning[:, :two] + burning[:, two:])
        fire = (fire + flat(heat[at, cell])) + 0.5 * x
        if second:
            fire = 0.5 * (fire + flat(v[at, inner]))
        target[at, inner] = fire.reshape(n, size, two)

    def pyramid(k, first=0, last=tiles):
        if k == d:
            first, last = max(first, 1), min(last, tiles - 1)
        low, count = d + k, own - k
        blocks = -(-count * (last - first) // LARGEST)
        for b in range(blocks):
            begin, end = count * b // blocks, count * (b + 1) // blocks
            evaluate(low + begin, end - begin, k % 2 == 0, first, last, top=b == blocks - 1)

    def take_ints():
        for s in range(2):
            for n in range(3):
                arrived(functools.partial(int_copy, n), s)
        late = []
        for ref in (fuel_ref, break_ref, lit_ref):
            late += [ref[0:group].astype(F32), ref[full - group:full].astype(F32)]
        flatten(jnp.concatenate(late, axis=0), 2 * group, [(groups, 0)])
        for s in (2, 3):
            start(functools.partial(flat_copy, 1), s)
        lax.fori_loop(0, d, cells, 0, unroll=4)

    def take_rows(j):
        for m in range(j * CHUNK, (j + 1) * CHUNK):
            for s in range(2):
                arrived(functools.partial(row_copy, m), s)
        for m in range(CHUNK):
            p = d - CHUNK * (j + 1) + m
            v[p, PAD + d:PAD + d + w] = jnp.concatenate([halo_x[1, p], halo_x[0, p]], axis=0).T
        for s in (2, 3):
            start(functools.partial(corner_copy, j), s)

    def turn_out(i):
        tall = v[d + i, PAD + d:PAD + d + w].T
        out_ref[pl.ds(i, c, stride=h), :] = tall[:c]
        out_ref[pl.ds(h - 1 - i, c, stride=h), :] = tall[c:]

    def zone(j):
        for s in (2, 3):
            sent(functools.partial(corner_copy, j), s)
            arrived(functools.partial(corner_copy, j), s)
        if j == 1:
            for i in range(d, own):
                turn_out(i)

        for k in range(1, d + 1):
            edge_tile = 1 if k == d else 0
            evaluate(d - CHUNK * (j + 1) + k, CHUNK, k % 2 == 0, edge_tile, tiles - edge_tile)

    for k in range(1, EARLY + 1):
        pyramid(k, k + 1, tiles - k - 1)
    take_ints()
    take_cols()
    relay()
    for m in range(own // TILE):
        for s in (2, 3):
            sent(functools.partial(col_copy, m), s)
    for k in range(1, EARLY + 1):
        pyramid(k, 0, k + 1)
        pyramid(k, tiles - k - 1, tiles)
    take_rows(0)
    for s in (2, 3):
        arrived(functools.partial(flat_copy, 1), s)
    edge_cells([(0, groups)])
    for k in range(EARLY + 1, d + 1):
        pyramid(k)
        if k == d - 1:
            take_rows(1)
    zone(0)

    zone(1)
    for i in range(d):
        turn_out(i)
    for s in range(2):
        for n in range(3):
            sent(functools.partial(int_copy, n), s)
        for j in range(d):
            sent(functools.partial(row_copy, j), s)
    for s in (2, 3):
        for late in range(2):
            sent(functools.partial(flat_copy, late), s)
    relayed()


def per_device(n_row, n_col, fire_state, fuel_class, firebreak, ignition, spread_rate, spread_rows, spread_cols, reaction, ignition_heat):
    c, h, w = fire_state.shape
    k = spread_rate.shape[0]
    k8 = -(-k // 8) * 8
    d = DEPTH
    own, two = h // 2, 2 * c
    total, wide = own + d, w + 2 * d
    groups = total * d // w
    field = pltpu.VMEM((total + 1, wide + 2 * PAD, two), F32)
    terms = pltpu.VMEM((total, wide, two), F32)
    ints = pltpu.VMEM((h + 2 * d, w), jnp.int32)
    dma = pltpu.SemaphoreType.DMA
    out = pl.pallas_call(
        functools.partial(kernel, (n_row, n_col, c, h, w, k8)),
        out_shape=pltpu.VMEM((c * h, w), F32),
        in_specs=[pl.BlockSpec(memory_space=pltpu.HBM)] * 9,
        out_specs=pl.BlockSpec(memory_space=pltpu.VMEM),
        scratch_shapes=[
            pltpu.VMEM((c * h, w), F32),
            ints, ints, ints,
            pltpu.VMEM(spread_rate.shape, F32),
            pltpu.VMEM((c, c), F32), pltpu.VMEM((c, c), F32), pltpu.VMEM((c, c), F32),
            pltpu.VMEM((1, c), F32),
            dma((9,)),
            field, field, terms, terms, terms,
            pltpu.VMEM((2 * two, 2 * two), BF16),
            pltpu.VMEM((2 * two, 2 * two), BF16),
            pltpu.VMEM((2 * (k8 + 8), 3 * two), F32),
            pltpu.VMEM((2, d, c, w), F32),
            pltpu.VMEM((d - CHUNK, c, w), F32),
            pltpu.VMEM((2, groups + 1, 8, w), F32),
            pltpu.VMEM((2, groups + 1, 8, w), F32),
            dma((d, 2)), dma((d, 2)), dma((3, 2)), dma((3, 2)), dma((own // TILE, 2)), dma((own // TILE, 2)), dma((2, 2)), dma((2, 2)),
            dma((d // CHUNK, 2)), dma((d // CHUNK, 2)),
            dma((d - CHUNK,)), dma((d - CHUNK,)),
        ],
        compiler_params=pltpu.CompilerParams(collective_id=0, has_side_effects=True, vmem_limit_bytes=56 * 1048576),
    )(
        fire_state, fuel_class, firebreak, ignition,
        spread_rate, spread_rows, spread_cols, reaction, ignition_heat.reshape(1, c),
    )
    return out.reshape(c, h, w)


def solution(mesh):
    grid = P("row", "col")
    field = P(None, "row", "col")
    return jax.shard_map(
        functools.partial(per_device, mesh.shape["row"], mesh.shape["col"]),
        mesh=mesh,
        in_specs=(field, grid, grid, grid, P(), P(), P(), P(), P()),
        out_specs=field,
        check_vma=False,
    )
```
